512 devices in a mesh: prow: 16 (over y, z_hi, core), pcol: 32 (over x, z_lo).
Axes of the slice: x: 4, y: 4, z: 16 (z_hi: 2, z_lo: 8; z = z_hi * 8 + z_lo), core: 2. Of those that a mesh axis runs over, the one named last changes fastest.
Arguments:
- tiles: bfloat16 [16, 32, 16, 256, 256], P('prow', 'pcol'), may hold values from -6 to 6
- tile_ids: int32 [16, 32, 16], P('prow', 'pcol'), may hold values from 0 to 127, as said below
- counts: int32 [16, 32], P('prow', 'pcol'), may hold values from 1 to 16, as said below
- pivots: int32 [256], replicated, may hold values from 0 to 65535, as said below
- l_inverse: bfloat16 [256, 256], P(None, 'pcol'), may hold values from -1 to 1, as said below
- u_inverse: bfloat16 [256, 256], P('prow'), may hold values from -0.125 to 0.5, as said below
Outputs:
- factored: bfloat16 [16, 32, 16, 256, 256], P('prow', 'pcol')
The draws below stay inside these ranges and needn't reach their ends.
Inputs may be any that keep to these rules, and one draw needn't show every extreme that they name: Live slot s of device (p, q) holds local tile row tile_ids[p, q, s] // 8 and local tile column tile_ids[p, q, s] % 8; live codes of one device are distinct, padded slots hold arbitrary codes. Let R be the tile rows I >= 1 with tile (I, 0) held and C the tile columns J >= 1 with tile (0, J) held. Tile (0, 0) is held; on each prow index R takes the last one to 3 local tile rows, on each pcol index C takes the last one to 3 local tile columns, and both most counts are reached on some index. Every tile whose row is 0 or in R and whose column is 0 or in C is held; no other held tile lies in tile row 0, a tile row of R, or tile column 0. `counts`: some device has 16 live slots. Row r of tile row 0 and row pivots[r] change places; pivots[r] is r or a row of a tile row of R, and the values that differ from their r are distinct. `l_inverse`: lower triangular with unit diagonal. `u_inverse`: upper triangular with a positive diagonal.
All inputs are finite; a program needn't handle non-finite values.
Results may differ from the reference program's by a relative error of at most 0.0056.
Values may be sent and summed in bfloat16 or wider, within the bound.
No kernel may reach another device: no remote copies, remote signals or barrier semaphores. Data moves between devices by JAX's collectives and lax.ppermute only.
A program may use at most 64 MiB of HBM per device.

```python
import jax
import jax.numpy as jnp
from jax import lax

TILE_SIDE = 256
LOCAL_ROWS = 16
LOCAL_COLS = 8
TILE_GRID = 256
TILE_SLOTS = 16
LOWER_MOST = 3
UPPER_MOST = 3
N_PROW = 16
N_PCOL = 32


def layout(key):
    base = jax.random.fold_in(key, 17)
    keys = jax.random.split(base, 9)
    prow_count = TILE_GRID // LOCAL_ROWS
    pcol_count = TILE_GRID // LOCAL_COLS
    positions = LOCAL_ROWS * LOCAL_COLS
    lower_count = jax.random.randint(keys[0], (prow_count,), 1, LOWER_MOST + 1)
    lower_count = lower_count.at[jax.random.randint(keys[1], (), 0, prow_count)].set(LOWER_MOST)
    upper_count = jax.random.randint(keys[2], (pcol_count,), 1, UPPER_MOST + 1)
    upper_count = upper_count.at[jax.random.randint(keys[3], (), 0, pcol_count)].set(UPPER_MOST)
    row_local = jnp.arange(LOCAL_ROWS, dtype=jnp.int32)
    col_local = jnp.arange(LOCAL_COLS, dtype=jnp.int32)
    lower_rows = row_local[None, :] >= LOCAL_ROWS - lower_count[:, None]
    upper_cols = col_local[None, :] >= LOCAL_COLS - upper_count[:, None]
    prow_first = (jnp.arange(prow_count)[:, None] == 0) & (row_local[None, :] == 0)
    pcol_first = (jnp.arange(pcol_count)[:, None] == 0) & (col_local[None, :] == 0)
    row_set = lower_rows | prow_first
    col_set = upper_cols | pcol_first
    grid_shape = (prow_count, pcol_count, LOCAL_ROWS, LOCAL_COLS)
    structural = jnp.broadcast_to(row_set[:, None, :, None] & col_set[None, :, None, :], grid_shape)
    free = jnp.broadcast_to((~row_set)[:, None, :, None] & (~pcol_first)[None, :, None, :], grid_shape)
    structural = structural.reshape(prow_count, pcol_count, positions)
    free = free.reshape(prow_count, pcol_count, positions)
    base_count = jnp.sum(structural.astype(jnp.int32), axis=2)
    room = TILE_SLOTS - base_count
    extra = jax.random.randint(keys[4], (prow_count, pcol_count), 0, room + 1)
    full_row = jax.random.randint(keys[5], (), 0, prow_count)
    full_col = jax.random.randint(keys[6], (), 0, pcol_count)
    extra = extra.at[full_row, full_col].set(room[full_row, full_col])
    place = jnp.arange(positions, dtype=jnp.int32)
    noise = jax.random.randint(keys[7], (prow_count, pcol_count, positions), 0, 2 ** 20)
    score = jnp.where(free, noise * positions + place, -1 - place)
    rank = jnp.argsort(jnp.argsort(-score, axis=2), axis=2)
    chosen = free & (rank < extra[:, :, None])
    present = structural | chosen
    noise_two = jax.random.randint(keys[8], (prow_count, pcol_count, positions), 0, 2 ** 20)
    order_score = jnp.where(present, noise_two * positions + place, -1 - place)
    codes = jnp.argsort(-order_score, axis=2)[:, :, :TILE_SLOTS].astype(jnp.int32)
    live_count = (base_count + extra).astype(jnp.int32)
    return (codes, live_count, lower_rows)


def draw_tile_ids(key, part):
    return layout(key)[0]


def draw_counts(key, part):
    return layout(key)[1]


def draw_pivots(key, part):
    lower_rows = layout(key)[2]
    prow_count = TILE_GRID // LOCAL_ROWS
    total_rows = TILE_GRID * TILE_SIDE
    rows = jnp.arange(total_rows, dtype=jnp.int32)
    tile_row = rows // TILE_SIDE
    eligible = lower_rows[tile_row % prow_count, tile_row // prow_count]
    keys = jax.random.split(jax.random.fold_in(key, 29), 2)
    noise = jax.random.randint(keys[0], (total_rows,), 0, 2 ** 14)
    score = jnp.where(eligible, noise * total_rows + rows, -1)
    picked = jnp.argsort(-score)[:TILE_SIDE].astype(jnp.int32)
    stay = jax.random.randint(keys[1], (TILE_SIDE,), 0, 5) == 0
    return jnp.where(stay, jnp.arange(TILE_SIDE, dtype=jnp.int32), picked)


def draw_l_inverse(key, part):
    first = jax.random.fold_in(jax.random.fold_in(key, 41), 0)
    below = jnp.clip(jax.random.normal(first, (TILE_SIDE, TILE_SIDE), jnp.float32), -4.0, 4.0)
    below = below / jnp.sqrt(jnp.float32(TILE_SIDE))
    return (jnp.tril(below, -1) + jnp.eye(TILE_SIDE, dtype=jnp.float32)).astype(jnp.bfloat16)


def draw_u_inverse(key, part):
    first, second = jax.random.split(jax.random.fold_in(key, 53))
    above = jnp.clip(jax.random.normal(first, (TILE_SIDE, TILE_SIDE), jnp.float32), -4.0, 4.0)
    diagonal = jnp.exp(jax.random.uniform(second, (TILE_SIDE,), jnp.float32, jnp.log(0.5), jnp.log(2.0)))
    above = above / jnp.sqrt(jnp.float32(TILE_SIDE))
    upper = jnp.triu(above, 1) + jnp.diag(diagonal)
    return (upper / 8.0).astype(jnp.bfloat16)


def block_levels(rng, extent, cuts, least, top_value):
    level = 1.0
    for dim, blocks in cuts:
        draws = jax.random.uniform(jax.random.fold_in(jax.random.fold_in(rng, 6), dim), (blocks,), jnp.float32, least / len(cuts), top_value / len(cuts))
        level = level * jnp.repeat(jnp.exp(draws), extent[dim] // blocks).reshape((-1,) + (1,) * (len(extent) - 1 - dim))
    return level


def gaussian(key, dims, deviation, most, shards=(), kind=jnp.bfloat16):
    level = block_levels(key, dims, shards, -0.22, 0.18) if shards else 1.0
    array = jax.random.normal(key, dims, jnp.float32) * deviation * level
    return jnp.minimum(jnp.maximum(array, -most), most).astype(kind)


def setup_inputs(seed: int = 0) -> dict:
    key_of = jax.random.split(jax.random.key(seed), 7)
    tiles = gaussian(key_of[0], (N_PROW, N_PCOL, TILE_SLOTS, TILE_SIDE, TILE_SIDE), 1.0, 6.0, ((0, 16), (1, 32)))
    tile_ids = draw_tile_ids(jax.random.fold_in(key_of[6], 71), 0)
    counts = draw_counts(jax.random.fold_in(key_of[6], 71), 0)
    pivots = draw_pivots(jax.random.fold_in(key_of[6], 71), 0)
    l_inverse = draw_l_inverse(jax.random.fold_in(key_of[6], 71), 0)
    u_inverse = draw_u_inverse(jax.random.fold_in(key_of[6], 71), 0)
    return {"tiles": tiles, "tile_ids": tile_ids, "counts": counts, "pivots": pivots, "l_inverse": l_inverse, "u_inverse": u_inverse}


def reference(tiles, tile_ids, counts, pivots, l_inverse, u_inverse):
    side = TILE_SIDE
    total_rows = TILE_GRID * side
    device_total = N_PROW * N_PCOL * TILE_SLOTS
    flat = tiles.reshape(device_total, side, side)
    flat_rows = flat.reshape(device_total * side, side)
    shape = tile_ids.shape
    prow_of = jnp.broadcast_to(jnp.arange(N_PROW, dtype=jnp.int32)[:, None, None], shape).reshape(-1)
    pcol_of = jnp.broadcast_to(jnp.arange(N_PCOL, dtype=jnp.int32)[None, :, None], shape).reshape(-1)
    slot_of = jnp.broadcast_to(jnp.arange(TILE_SLOTS, dtype=jnp.int32)[None, None, :], shape).reshape(-1)
    alive = slot_of < jnp.broadcast_to(counts[:, :, None], shape).reshape(-1)
    codes = tile_ids.reshape(-1)
    glob_row = (prow_of + N_PROW * (codes // LOCAL_COLS)).astype(jnp.int32)
    glob_col = (pcol_of + N_PCOL * (codes % LOCAL_COLS)).astype(jnp.int32)
    table = jnp.full((TILE_GRID, TILE_GRID), -1, jnp.int32)
    table = table.at[jnp.where(alive, glob_row, TILE_GRID), glob_col].set(
        jnp.arange(device_total, dtype=jnp.int32), mode="drop")

    def fetch(slot, row):
        picked = flat_rows[jnp.maximum(slot, 0) * side + row]
        return jnp.where((slot >= 0)[..., None], picked, jnp.zeros_like(picked))

    every_col = jnp.arange(TILE_GRID, dtype=jnp.int32)
    row_range = jnp.arange(side, dtype=jnp.int32)
    new_slots = table[(pivots // side)[None, :], every_col[:, None]]
    new_top = fetch(new_slots, (pivots % side)[None, :])
    old_slots = jnp.broadcast_to(table[0, :][:, None], (TILE_GRID, side))
    old_top = fetch(old_slots, row_range[None, :])
    anchor_top = jnp.full((total_rows,), -1, jnp.int32).at[pivots].set(row_range)

    def primed_tile(tile, trow, tcol):
        anchor = lax.dynamic_slice_in_dim(anchor_top, (trow * side).astype(jnp.int32), side)
        moved = (anchor >= 0) & (trow >= 1)
        from_top = old_top[tcol][jnp.maximum(anchor, 0)]
        swapped = jnp.where(moved[:, None], from_top, tile)
        return jnp.where(trow == 0, new_top[tcol], swapped)

    lower_slot = table[:, 0]
    upper_slot = table[0, :]
    lower_present = (lower_slot >= 0) & (every_col >= 1)
    upper_present = (upper_slot >= 0) & (every_col >= 1)

    def lower_one(index):
        slot = lower_slot[index]
        tile = flat[jnp.maximum(slot, 0)]
        primed = primed_tile(tile, index, jnp.int32(0))
        value = jnp.dot(primed, u_inverse, preferred_element_type=jnp.float32).astype(jnp.bfloat16)
        return jnp.where(lower_present[index], value, jnp.zeros_like(value))

    def upper_one(index):
        value = jnp.dot(l_inverse, new_top[index], preferred_element_type=jnp.float32).astype(jnp.bfloat16)
        return jnp.where(upper_present[index], value, jnp.zeros_like(value))

    lower_panel = lax.map(lower_one, every_col)
    upper_row = lax.map(upper_one, every_col)

    def finish(index):
        tile = flat[index]
        trow = glob_row[index]
        tcol = glob_col[index]
        primed = primed_tile(tile, trow, tcol)

        def updated(unused):
            product = jnp.dot(lower_panel[trow], upper_row[tcol], preferred_element_type=jnp.float32)
            return (primed.astype(jnp.float32) - product).astype(jnp.bfloat16)

        def kept(unused):
            return primed

        interior = lax.cond(lower_present[trow] & upper_present[tcol], updated, kept, 0)
        value = jnp.where(trow == 0, jnp.where(tcol == 0, primed, upper_row[tcol]),
                          jnp.where(tcol == 0, lower_panel[trow], interior))
        return jnp.where(alive[index], value, jnp.zeros_like(value))

    result = lax.map(finish, jnp.arange(device_total, dtype=jnp.int32))
    return result.reshape(tiles.shape)
```

```python
import jax
import jax.numpy as jnp
from jax import lax
from jax.experimental import pallas as pl
from jax.experimental.pallas import tpu as pltpu
from jax.sharding import Mesh
from jax.sharding import PartitionSpec as P

SIDE = 256
SLOTS = 16
ROWS = 16
COLS = 8
LOWER = 3
UPPER = 3
LISTED = UPPER + 1
N_ROW = 16
N_X = 4
N_Z = 8
CHUNK = SIDE // N_ROW
PART = SIDE // N_X
PCOL = ("x", "zl")
EVERY = ("prow", "x", "zl")
BF = jnp.bfloat16
F32 = jnp.float32

SMEM = pl.BlockSpec(memory_space=pltpu.SMEM)
VMEM = pl.BlockSpec(memory_space=pltpu.VMEM)


def iota(dim):
    return lax.broadcasted_iota(jnp.int32, (SIDE, SIDE), dim)


def hot(mask):
    return jnp.where(mask, 1.0, 0.0).astype(BF)


def times(a, b):
    return jnp.dot(a, b, preferred_element_type=F32)


def slot_of(meta, s):
    code = meta[s]
    return code // COLS, code % COLS, s < meta[SLOTS], meta[SLOTS + 1], meta[SLOTS + 2]


def listed_column(col, q):
    return (col >= COLS - UPPER) | ((col == 0) & (q == 0)), jnp.where(col == 0, UPPER, COLS - 1 - col)


def spread_rows(pivots):
    return jnp.transpose(jnp.broadcast_to(pivots, (SIDE, SIDE)))


def give_kernel(meta, pivots, tiles, out, total):
    total[...] = jnp.zeros_like(total)
    piv = spread_rows(pivots[...])
    lane, sub = iota(1), iota(0)
    leaves = (piv // SIDE) % N_ROW != 0

    def step(s, carry):
        row, col, live, p, q = slot_of(meta, s)
        takes, k = listed_column(col, q)
        top = (row == 0) & (p == 0)

        @pl.when(live & takes & (top | (row >= ROWS - LOWER)))
        def _():
            wanted = piv - SIDE * (p + N_ROW * row)
            wanted = jnp.where(leaves & top, sub, wanted)
            total[k] += times(hot(wanted == lane), tiles[s])

        return carry

    lax.fori_loop(0, SLOTS, step, 0)
    for k in range(LISTED):
        out[:, k] = total[k].astype(BF).reshape(N_ROW, CHUNK, SIDE)


def relay_kernel(meta, owners, got, upper, lower, out):
    p = meta[SLOTS + 1]
    sub = lax.broadcasted_iota(jnp.int32, (CHUNK, SIDE), 0)
    mine = jnp.zeros((CHUNK, SIDE), jnp.int32)
    for r in range(CHUNK):
        mine = jnp.where(sub == r, owners[p * CHUNK + r], mine)
    owner = jnp.broadcast_to(mine[None], (N_ROW, CHUNK, SIDE)).reshape(SIDE, SIDE)
    to, frm = iota(0), iota(1)
    source = jnp.where(owner == to // CHUNK, 0, owner)
    pick = hot((to % CHUNK == frm % CHUNK) & (frm // CHUNK == source))
    for k in range(LISTED):
        rows = got[:, k].reshape(SIDE, SIDE)
        out[:, k] = times(pick, rows).astype(BF).reshape(N_ROW, CHUNK, SIDE)
    out[:, LISTED] = jnp.broadcast_to(upper[...][None], (N_ROW, CHUNK, SIDE))
    out[:, LISTED + 1] = jnp.broadcast_to(lower[...][None], (N_ROW, CHUNK, SIDE))


def swap_in(pivots, old, tile, first):
    match = pivots - first == iota(0)
    moved = jnp.max(jnp.where(match, 1.0, 0.0), axis=1, keepdims=True) > 0.0
    return jnp.where(moved, times(hot(match), old), tile.astype(F32)).astype(BF)


def solve_kernel(meta, pivots, tiles, got, out, old):
    q = meta[SLOTS + 2]

    @pl.when(q == 0)
    def _():
        out[...] = jnp.zeros_like(out)
        piv = jnp.broadcast_to(pivots[...], (SIDE, SIDE))
        inverse = got[:, LISTED].reshape(SIDE, SIDE)
        old[...] = got[:, UPPER].reshape(SIDE, SIDE)

        def top(s, carry):
            row, col, live, p, _ = slot_of(meta, s)

            @pl.when(live & (col == 0) & (row == 0) & (p == 0))
            def _():
                old[...] = tiles[s]

            return carry

        lax.fori_loop(0, SLOTS, top, 0)

        def step(s, carry):
            row, col, live, p, _ = slot_of(meta, s)

            @pl.when(live & (col == 0) & (row >= ROWS - LOWER))
            def _():
                swapped = swap_in(piv, old[...], tiles[s], SIDE * (p + N_ROW * row))
                solved = times(swapped, inverse).astype(BF)
                for c in range(N_X):
                    out[c, ROWS - 1 - row] = solved[c * PART : (c + 1) * PART]

            return carry

        lax.fori_loop(0, SLOTS, step, 0)


def ready_kernel(meta, pivots, tiles, gave, got, lower, out, upper, old, new):
    p, q = meta[SLOTS + 1], meta[SLOTS + 2]
    piv = jnp.broadcast_to(pivots[...], (SIDE, SIDE))
    own = (spread_rows(pivots[...]) // SIDE) % N_ROW == p
    j = iota(1)
    place = COLS * ((q - j // CHUNK - N_ROW * ((j // COLS) % 2)) % (N_X * N_Z)) + j % COLS
    inverse = times(hot(place == iota(0)), got[:, LISTED + 1].reshape(SIDE, SIDE)).astype(BF)
    for k in range(LISTED):
        theirs = got[:, k].reshape(SIDE, SIDE)
        ours = gave[:, k].reshape(SIDE, SIDE)
        old[k] = theirs
        new[k] = jnp.where(own, ours.astype(F32), theirs.astype(F32)).astype(BF)
    for k in range(UPPER):
        upper[k] = lax.dot_general(
            inverse, new[k], (((0,), (0,)), ((), ())), preferred_element_type=F32
        ).astype(BF)

    def top(s, carry):
        row, col, live, _, _ = slot_of(meta, s)
        takes, k = listed_column(col, q)

        @pl.when(live & takes & (row == 0) & (p == 0))
        def _():
            old[k] = tiles[s]

        return carry

    lax.fori_loop(0, SLOTS, top, 0)

    def step(s, carry):
        row, col, live, _, _ = slot_of(meta, s)
        takes, k = listed_column(col, q)
        first = (col == 0) & (q == 0)
        is_top = live & (row == 0) & (p == 0)
        is_lower = live & first & jnp.logical_not(is_top)
        is_swap = live & takes & jnp.logical_not(first) & (row >= ROWS - LOWER)
        is_kept = live & jnp.logical_not(is_top | is_lower | is_swap)

        @pl.when(is_top & first)
        def _():
            out[s] = new[UPPER]

        @pl.when(is_top & jnp.logical_not(first))
        def _():
            out[s] = upper[jnp.minimum(k, UPPER - 1)]

        @pl.when(is_lower)
        def _():
            for c in range(N_X):
                out[s, c * PART : (c + 1) * PART] = lower[c, jnp.minimum(ROWS - 1 - row, LOWER - 1)]

        @pl.when(is_swap)
        def _():
            out[s] = swap_in(piv, old[k], tiles[s], SIDE * (p + N_ROW * row))

        @pl.when(is_kept)
        def _():
            out[s] = tiles[s]

        @pl.when(jnp.logical_not(live))
        def _():
            out[s] = jnp.zeros((SIDE, SIDE), BF)

        return carry

    lax.fori_loop(0, SLOTS, step, 0)


def trail_kernel(meta, ready, upper, lower, out):
    def step(s, carry):
        row, col, live, _, _ = slot_of(meta, s)
        trails = live & (row >= ROWS - LOWER) & (col >= COLS - UPPER)

        @pl.when(trails)
        def _():
            left = jnp.concatenate([lower[c, ROWS - 1 - row] for c in range(N_X)], axis=0)
            product = times(left, upper[COLS - 1 - col])
            out[s] = (ready[s].astype(F32) - product).astype(BF)

        @pl.when(jnp.logical_not(trails))
        def _():
            out[s] = ready[s]

        return carry

    lax.fori_loop(0, SLOTS, step, 0)


def call(kernel, ins, outs, scratch=()):
    shapes = [jax.ShapeDtypeStruct(o, BF) for o in outs]
    return pl.pallas_call(
        kernel,
        out_shape=shapes if len(shapes) > 1 else shapes[0],
        in_specs=[SMEM if smem else VMEM for smem, _ in ins],
        out_specs=[VMEM] * len(shapes) if len(shapes) > 1 else VMEM,
        scratch_shapes=list(scratch),
        name=kernel.__name__,
    )(*[a for _, a in ins])


def exchange(blocks):
    flat = blocks.reshape(N_ROW, -1, SIDE)
    return lax.all_to_all(flat, "prow", 0, 0, tiled=True).reshape(blocks.shape)


def body(tiles, tile_ids, counts, pivots, l_inverse, u_inverse):
    p = lax.axis_index("prow").astype(jnp.int32)
    x = lax.axis_index("x").astype(jnp.int32)
    z = lax.axis_index("zl").astype(jnp.int32)
    q = x * N_Z + z
    local = tiles[0, 0]
    meta = jnp.concatenate([tile_ids[0, 0], counts[0], p[None], q[None]])
    owners = (pivots // SIDE) % N_ROW
    lanes = pivots[None]

    piece = l_inverse.T
    n_col = N_X * N_Z
    pieces = [
        lax.ppermute(
            piece,
            EVERY,
            [(a * n_col + b, a * n_col + (b + a + N_ROW * h) % n_col) for a in range(N_ROW) for b in range(n_col)],
        )
        for h in range(2)
    ]
    brought = jnp.concatenate(pieces, axis=0)

    stack = (N_ROW, LISTED, CHUNK, SIDE)
    gave = call(give_kernel, [(1, meta), (0, lanes), (0, local)], [stack], [pltpu.VMEM((LISTED, SIDE, SIDE), F32)])
    got = exchange(gave)
    relayed = call(
        relay_kernel,
        [(1, meta), (1, owners), (0, got), (0, u_inverse), (0, brought)],
        [(N_ROW, LISTED + 2, CHUNK, SIDE)],
    )
    have = exchange(relayed)

    parts = call(
        solve_kernel,
        [(1, meta), (0, lanes), (0, local), (0, have)],
        [(N_X, LOWER, PART, SIDE)],
        [pltpu.VMEM((SIDE, SIDE), BF)],
    )
    part = parts[0]
    for c in range(1, N_X):
        sent = lax.ppermute(parts[c], PCOL, [(0, c * N_Z)])
        part = jnp.where(x == c, sent, part)
    for step in (4, 2, 1):
        sent = lax.ppermute(part, "zl", [(a, a + step) for a in range(0, N_Z, 2 * step)])
        part = jnp.where(z % (2 * step) == step, sent, part)
    lower = lax.all_to_all(
        jnp.broadcast_to(part[None], (N_X, LOWER, PART, SIDE)), "x", 0, 0, tiled=True
    )

    ready, upper = call(
        ready_kernel,
        [(1, meta), (0, lanes), (0, local), (0, gave), (0, have), (0, parts)],
        [(SLOTS, SIDE, SIDE), (UPPER, SIDE, SIDE)],
        [pltpu.VMEM((LISTED, SIDE, SIDE), BF), pltpu.VMEM((LISTED, SIDE, SIDE), BF)],
    )
    result = call(
        trail_kernel, [(1, meta), (0, ready), (0, upper), (0, lower)], [(SLOTS, SIDE, SIDE)]
    )
    return result[None, None]


def solution(mesh):
    torus = Mesh(mesh.devices.reshape(N_ROW, N_X, N_Z), EVERY)
    placed = (
        P("prow", PCOL, None, None, None),
        P("prow", PCOL, None),
        P("prow", PCOL),
        P(),
        P(None, PCOL),
        P("prow", None),
    )
    return jax.shard_map(
        body,
        mesh=torus,
        in_specs=placed,
        out_specs=P("prow", PCOL, None, None, None),
        check_vma=False,
    )
```

```python
import jax
import jax.numpy as jnp
from jax import lax
from jax.experimental import pallas as pl
from jax.experimental.pallas import tpu as pltpu
from jax.sharding import Mesh
from jax.sharding import PartitionSpec as P

SIDE = 256
SLOTS = 16
ROWS = 16
COLS = 8
LOWER = 3
UPPER = 3
LISTED = UPPER + 1
N_ROW = 16
N_Y = 4
N_PLANE = 8
N_X = 4
N_Z = 8
CHUNK = SIDE // N_PLANE
PIECE = SIDE // N_ROW
PART = SIDE // N_X
GIVEN = LISTED * CHUNK
SENT = GIVEN + 2 * PIECE
PANEL = LOWER * PART
PROW = ("y", "zh", "core")
PCOL = ("x", "zl")
BF = jnp.bfloat16
F32 = jnp.float32

SMEM = pl.BlockSpec(memory_space=pltpu.SMEM)
VMEM = pl.BlockSpec(memory_space=pltpu.VMEM)
ANY = pl.BlockSpec(memory_space=pl.ANY)


def iota(dim, rows=SIDE):
    return lax.broadcasted_iota(jnp.int32, (rows, SIDE), dim)


def hot(mask):
    return jnp.where(mask, 1.0, 0.0).astype(BF)


def times(a, b):
    return jnp.dot(a, b, preferred_element_type=F32)


def row_of():
    return (lax.axis_index("y") * 2 + lax.axis_index("zh")) * 2 + lax.axis_index("core")


def col_of():
    return lax.axis_index("x") * N_Z + lax.axis_index("zl")


def slot_of(ids, counts, s):
    code = ids[0, 0, s]
    return code // COLS, code % COLS, s < counts[0, 0]


def listed_column(col, q):
    return (col >= COLS - UPPER) | ((col == 0) & (q == 0)), jnp.where(col == 0, UPPER, COLS - 1 - col)


def spread_rows(pivots):
    return jnp.transpose(jnp.broadcast_to(pivots, (SIDE, SIDE)))


def block_rows(block, k):
    return block[:, k * CHUNK : (k + 1) * CHUNK].reshape(SIDE, SIDE)


def give_kernel(ids, counts, pivots, tiles, out, held, here, sems):
    p, q = row_of(), col_of()
    for i in range(LOWER + 1):
        for k in range(LISTED):
            here[i, k] = 0

    def place(s):
        row, col, live = slot_of(ids, counts, s)
        takes, k = listed_column(col, q)
        top = (row == 0) & (p == 0)
        i = jnp.where(top, LOWER, ROWS - 1 - row)
        return live & takes & (top | (row >= ROWS - LOWER)), i, k

    for s in range(SLOTS):
        wanted, i, k = place(s)

        @pl.when(wanted)
        def _():
            here[i, k] = 1
            pltpu.make_async_copy(tiles.at[0, 0, s], held.at[k, i], sems.at[s]).start()

    for i in range(LOWER + 1):
        for k in range(LISTED):

            @pl.when(here[i, k] == 0)
            def _():
                held[k, i] = jnp.zeros((SIDE, SIDE), BF)

    piv = spread_rows(pivots[...])
    lane, sub = iota(1), iota(0)
    leaves = ((piv // SIDE) % N_ROW != 0) & (p == 0)
    picks = [hot(piv - SIDE * (p + N_ROW * (ROWS - 1 - i)) == lane) for i in range(LOWER)]
    picks.append(hot(jnp.where(leaves, sub, piv - SIDE * p) == lane))
    pick = jnp.concatenate(picks, axis=1)

    for s in range(SLOTS):
        wanted, i, k = place(s)

        @pl.when(wanted)
        def _():
            pltpu.make_async_copy(tiles.at[0, 0, s], held.at[k, i], sems.at[s]).wait()

    for k in range(LISTED):
        rows = times(pick, held[k].reshape((LOWER + 1) * SIDE, SIDE)).astype(BF)
        out[:, k * CHUNK : (k + 1) * CHUNK] = rows.reshape(N_PLANE, CHUNK, SIDE)


def chunk_owner(pivots):
    first = (lax.axis_index("y") * 2 + lax.axis_index("core")) * CHUNK
    sub = iota(0, CHUNK)
    owner = jnp.zeros((CHUNK, SIDE), jnp.int32)
    for r in range(CHUNK):
        owner = jnp.where(sub == r, (pivots[first + r] // SIDE) % N_ROW, owner)
    return (owner // 2) % 2 == lax.axis_index("zh"), owner // 4 * 2 + owner % 2


def cross_kernel(pivots, got, upper, out):
    near, place = chunk_owner(pivots)
    frm = iota(1, CHUNK)
    pick = hot((iota(0, CHUNK) == frm % CHUNK) & (frm // CHUNK == jnp.where(near, place, 0)))
    for k in range(LISTED):
        out[k * CHUNK : (k + 1) * CHUNK] = times(pick, block_rows(got, k)).astype(BF)
    out[GIVEN:] = upper[...]


def relay_kernel(pivots, got, theirs, upper, out):
    zh = lax.axis_index("zh")
    near, place = chunk_owner(pivots)

    def wide(v):
        v = jnp.where(v, 1, 0) if v.dtype == jnp.bool_ else v
        return jnp.broadcast_to(v[None], (N_PLANE, CHUNK, SIDE)).reshape(SIDE, SIDE)

    near, place = wide(near) == 1, wide(place)
    to, frm = iota(0), iota(1)
    mine = to // CHUNK == place
    far = jnp.logical_not(near) | (mine & (zh == 1))
    source = jnp.where(mine, 0, place)
    pick = hot((to % CHUNK == frm % CHUNK) & (frm // CHUNK == source) & jnp.logical_not(far))
    for k in range(LISTED):
        other = theirs[k * CHUNK : (k + 1) * CHUNK].astype(F32)
        other = jnp.broadcast_to(other[None], (N_PLANE, CHUNK, SIDE)).reshape(SIDE, SIDE)
        rows = jnp.where(far, other, times(pick, block_rows(got, k))).astype(BF)
        out[:, k * CHUNK : (k + 1) * CHUNK] = rows.reshape(N_PLANE, CHUNK, SIDE)
    ours, others = upper[...].astype(F32), theirs[GIVEN:].astype(F32)
    for h in range(2):
        rows = jnp.where(zh == h, ours, others).astype(BF)
        out[:, GIVEN + h * PIECE : GIVEN + (h + 1) * PIECE] = jnp.broadcast_to(
            rows[None], (N_PLANE, PIECE, SIDE)
        )


def swap_in(pivots, old, tile, first):
    match = pivots - first == iota(0)
    moved = jnp.max(jnp.where(match, 1.0, 0.0), axis=1, keepdims=True) > 0.0
    return jnp.where(moved, times(hot(match), old), tile.astype(F32)).astype(BF)


def solve_kernel(ids, counts, pivots, tiles, got, *rest):
    outs, (inverse, old, held, here, sems) = rest[:N_X], rest[N_X:]
    p, q = row_of(), col_of()

    @pl.when(q == 0)
    def _():
        for i in range(LOWER + 1):
            here[i] = 0

        def place(s):
            row, col, live = slot_of(ids, counts, s)
            top = (row == 0) & (p == 0)
            i = jnp.where(top, LOWER, ROWS - 1 - row)
            return live & (col == 0) & (top | (row >= ROWS - LOWER)), i

        for s in range(SLOTS):
            wanted, i = place(s)

            @pl.when(wanted)
            def _():
                here[i] = 1
                pltpu.make_async_copy(tiles.at[0, 0, s], held.at[i], sems.at[s]).start()

        for y in range(N_Y):
            for h in range(2):
                for c in range(2):
                    r = (4 * y + 2 * h + c) * PIECE
                    a = GIVEN + h * PIECE
                    inverse[r : r + PIECE] = got[2 * y + c, a : a + PIECE]
        piv = jnp.broadcast_to(pivots[...], (SIDE, SIDE))
        old[...] = block_rows(got, UPPER)

        for s in range(SLOTS):
            wanted, i = place(s)

            @pl.when(wanted)
            def _():
                pltpu.make_async_copy(tiles.at[0, 0, s], held.at[i], sems.at[s]).wait()

        @pl.when(here[LOWER] == 1)
        def _():
            old[...] = held[LOWER]

        for i in range(LOWER):

            @pl.when(here[i] == 1)
            def _():
                swapped = swap_in(piv, old[...], held[i], SIDE * (p + N_ROW * (ROWS - 1 - i)))
                solved = times(swapped, inverse[...]).astype(BF)
                for c in range(N_X):
                    outs[c][i * PART : (i + 1) * PART] = solved[c * PART : (c + 1) * PART]

            @pl.when(here[i] == 0)
            def _():
                for c in range(N_X):
                    outs[c][i * PART : (i + 1) * PART] = jnp.zeros((PART, SIDE), BF)


def ready_kernel(ids, counts, pivots, tiles, gave, got, l0, l1, l2, l3, out, new, old):
    lower = (l0, l1, l2, l3)
    p, q = row_of(), col_of()
    piv = jnp.broadcast_to(pivots[...], (SIDE, SIDE))
    own = (spread_rows(pivots[...]) // SIDE) % N_ROW == p
    for k in range(LISTED):
        theirs = block_rows(got, k)
        ours = block_rows(gave, k)
        old[k] = theirs
        new[k] = jnp.where(own, ours.astype(F32), theirs.astype(F32)).astype(BF)

    def top(s, carry):
        row, col, live = slot_of(ids, counts, s)
        takes, k = listed_column(col, q)

        @pl.when(live & takes & (row == 0) & (p == 0))
        def _():
            old[k] = tiles[0, 0, s]

        return carry

    lax.fori_loop(0, SLOTS, top, 0)

    def step(s, carry):
        row, col, live = slot_of(ids, counts, s)
        takes, k = listed_column(col, q)
        first = (col == 0) & (q == 0)
        is_top = live & (row == 0) & (p == 0)
        is_lower = live & first & jnp.logical_not(is_top)
        is_swap = live & takes & jnp.logical_not(first) & (row >= ROWS - LOWER)
        is_kept = live & jnp.logical_not(is_top | is_lower | is_swap)

        @pl.when(is_top & first)
        def _():
            out[s] = new[UPPER]

        @pl.when(is_lower)
        def _():
            start = pl.multiple_of(jnp.clip(ROWS - 1 - row, 0, LOWER - 1) * PART, PART)
            for c in range(N_X):
                out[s, c * PART : (c + 1) * PART] = lower[c][pl.ds(start, PART)]

        @pl.when(is_swap)
        def _():
            out[s] = swap_in(piv, old[k], tiles[0, 0, s], SIDE * (p + N_ROW * row))

        @pl.when(is_kept)
        def _():
            out[s] = tiles[0, 0, s]

        @pl.when(jnp.logical_not(live))
        def _():
            out[s] = jnp.zeros((SIDE, SIDE), BF)

        return carry

    lax.fori_loop(0, SLOTS, step, 0)


def trail_kernel(ids, counts, ready, new, panel, out, held, left, upper, sems, back):
    p = row_of()

    def place(s):
        row, col, live = slot_of(ids, counts, s)
        listed = live & (col >= COLS - UPPER)
        top = listed & (row == 0) & (p == 0)
        i = jnp.clip(ROWS - 1 - row, 0, LOWER - 1)
        k = jnp.clip(COLS - 1 - col, 0, UPPER - 1)
        return top, listed & (row >= ROWS - LOWER), i, k

    for s in range(SLOTS):
        _, trails, _, _ = place(s)

        @pl.when(trails)
        def _():
            pltpu.make_async_copy(ready.at[0, 0, s], held.at[s], sems.at[s]).start()

    j = iota(1)
    e, t = j // COLS % N_Z, j % COLS
    e = (e % 2) * 4 + e // 2 % 2 * 2 + e // 4
    mine = j // PART * PART + COLS * (e ^ lax.axis_index("zl")) + t
    pieces = panel[:, PANEL:].reshape(SIDE, SIDE)
    inverse = times(hot(mine == iota(0)), pieces).astype(BF)
    for k in range(UPPER):
        upper[k] = lax.dot_general(
            inverse, new[k], (((0,), (0,)), ((), ())), preferred_element_type=F32
        ).astype(BF)
    for i in range(LOWER):
        left[i] = panel[:, i * PART : (i + 1) * PART].reshape(SIDE, SIDE)

    for s in range(SLOTS):
        top, trails, i, k = place(s)

        @pl.when(top)
        def _():
            held[s] = upper[k]

        @pl.when(trails)
        def _():
            pltpu.make_async_copy(ready.at[0, 0, s], held.at[s], sems.at[s]).wait()
            held[s] = (held[s].astype(F32) - times(left[i], upper[k])).astype(BF)

        @pl.when(top | trails)
        def _():
            pltpu.make_async_copy(held.at[s], out.at[0, 0, s], back.at[s]).start()

    for s in range(SLOTS):
        top, trails, _, _ = place(s)

        @pl.when(top | trails)
        def _():
            pltpu.make_async_copy(held.at[s], out.at[0, 0, s], back.at[s]).wait()


def call(kernel, specs, ins, shapes, scratch=(), out_space=VMEM, aliases=None):
    shapes = [jax.ShapeDtypeStruct(o, BF) for o in shapes]
    several = len(shapes) > 1
    return pl.pallas_call(
        kernel,
        out_shape=shapes if several else shapes[0],
        in_specs=[{"s": SMEM, "v": VMEM, "a": ANY}[c] for c in specs],
        out_specs=[out_space] * len(shapes) if several else out_space,
        scratch_shapes=list(scratch),
        input_output_aliases=aliases or {},
        name=kernel.__name__,
    )(*ins)


def body(tiles, tile_ids, counts, pivots, l_inverse, u_inverse):
    x = lax.axis_index("x")
    z = lax.axis_index("zl")
    lanes = pivots[None]
    tile = (SIDE, SIDE)
    plane = ("y", "core")

    gave = call(
        give_kernel,
        "ssva",
        [tile_ids, counts, lanes, tiles],
        [(N_PLANE, GIVEN, SIDE)],
        [
            pltpu.VMEM((LISTED, LOWER + 1, SIDE, SIDE), BF),
            pltpu.SMEM((LOWER + 1, LISTED), jnp.int32),
            pltpu.SemaphoreType.DMA((SLOTS,)),
        ],
    )
    got = lax.all_to_all(gave, plane, 0, 0, tiled=True)
    crossing = call(cross_kernel, "svv", [pivots, got, u_inverse], [(GIVEN + PIECE, SIDE)])
    theirs = lax.ppermute(crossing, "zh", [(0, 1), (1, 0)])
    relayed = call(
        relay_kernel, "svvv", [pivots, got, theirs, u_inverse], [(N_PLANE, SENT, SIDE)]
    )
    have = lax.all_to_all(relayed, plane, 0, 0, tiled=True)

    parts = call(
        solve_kernel,
        "ssvav",
        [tile_ids, counts, lanes, tiles, have],
        [(PANEL, SIDE)] * N_X,
        [
            pltpu.VMEM(tile, BF),
            pltpu.VMEM(tile, BF),
            pltpu.VMEM((LOWER + 1, SIDE, SIDE), BF),
            pltpu.SMEM((LOWER + 1,), jnp.int32),
            pltpu.SemaphoreType.DMA((SLOTS,)),
        ],
    )
    *parts, pieces = lax.optimization_barrier((*parts, l_inverse.T))
    part = parts[0]
    for c in range(1, N_X):
        sent = lax.ppermute(parts[c], PCOL, [(0, c * N_Z)])
        part = jnp.where(x == c, sent, part)
    for step in (4, 2, 1):
        sent = lax.ppermute(part, "zl", [(a, a + step) for a in range(0, N_Z, 2 * step)])
        part = jnp.where(z % (2 * step) == step, sent, part)
        more = lax.ppermute(pieces, "zl", [(a, a ^ step) for a in range(N_Z)])
        pieces = jnp.concatenate([pieces, more], axis=0)
    block = jnp.concatenate([part, pieces], axis=0)
    panel = lax.all_to_all(
        jnp.broadcast_to(block[None], (N_X, SIDE, SIDE)), "x", 0, 0, tiled=True
    )

    ready, new = call(
        ready_kernel,
        "ssvvvvvvvv",
        [tile_ids, counts, lanes, tiles, gave, have, *parts],
        [(SLOTS, SIDE, SIDE), (LISTED, SIDE, SIDE)],
        [pltpu.VMEM((LISTED, SIDE, SIDE), BF)],
    )
    return call(
        trail_kernel,
        "ssavv",
        [tile_ids, counts, ready[None, None], new, panel],
        [(1, 1, SLOTS, SIDE, SIDE)],
        [
            pltpu.VMEM((SLOTS, SIDE, SIDE), BF),
            pltpu.VMEM((LOWER, SIDE, SIDE), BF),
            pltpu.VMEM((UPPER, SIDE, SIDE), BF),
            pltpu.SemaphoreType.DMA((SLOTS,)),
            pltpu.SemaphoreType.DMA((SLOTS,)),
        ],
        out_space=ANY,
        aliases={2: 0},
    )


def solution(mesh):
    torus = Mesh(mesh.devices.reshape(N_Y, 2, 2, N_X, N_Z), PROW + PCOL)
    placed = (
        P(PROW, PCOL, None, None, None),
        P(PROW, PCOL, None),
        P(PROW, PCOL),
        P(),
        P(None, PCOL),
        P(PROW, None),
    )
    return jax.shard_map(
        body,
        mesh=torus,
        in_specs=placed,
        out_specs=P(PROW, PCOL, None, None, None),
        check_vma=False,
    )
```

```python
import jax
import jax.numpy as jnp
from jax import lax
from jax.experimental import pallas as pl
from jax.experimental.pallas import tpu as pltpu
from jax.sharding import Mesh
from jax.sharding import PartitionSpec as P

SIDE = 256
SLOTS = 16
ROWS = 16
COLS = 8
LOWER = 3
UPPER = 3
LISTED = UPPER + 1
N_ROW = 16
N_Y = 4
N_PLANE = 8
N_X = 4
N_Z = 8
CHUNK = SIDE // N_PLANE
PIECE = SIDE // N_ROW
PART = SIDE // N_X
GIVEN = LISTED * CHUNK
SENT = GIVEN + 2 * PIECE
PANEL = LOWER * PART
PROW = ("y", "zh", "core")
PCOL = ("x", "zl")
BF = jnp.bfloat16
F32 = jnp.float32

SMEM = pl.BlockSpec(memory_space=pltpu.SMEM)
VMEM = pl.BlockSpec(memory_space=pltpu.VMEM)
ANY = pl.BlockSpec(memory_space=pl.ANY)


def iota(dim, rows=SIDE):
    return lax.broadcasted_iota(jnp.int32, (rows, SIDE), dim)


def hot(mask):
    return jnp.where(mask, 1.0, 0.0).astype(BF)


def times(a, b):
    return jnp.dot(a, b, preferred_element_type=F32)


def row_of():
    return (lax.axis_index("y") * 2 + lax.axis_index("zh")) * 2 + lax.axis_index("core")


def col_of():
    return lax.axis_index("x") * N_Z + lax.axis_index("zl")


def slot_of(ids, counts, s):
    code = ids[0, 0, s]
    return code // COLS, code % COLS, s < counts[0, 0]


def listed_column(col, q):
    return (col >= COLS - UPPER) | ((col == 0) & (q == 0)), jnp.where(col == 0, UPPER, COLS - 1 - col)


def spread_rows(pivots):
    return jnp.transpose(jnp.broadcast_to(pivots, (SIDE, SIDE)))


def block_rows(block, k):
    return block[:, k * CHUNK : (k + 1) * CHUNK].reshape(SIDE, SIDE)


def give_kernel(ids, counts, pivots, tiles, out, held, here, sems):
    p, q = row_of(), col_of()
    for i in range(LOWER + 1):
        for k in range(LISTED):
            here[i, k] = 0

    def place(s):
        row, col, live = slot_of(ids, counts, s)
        takes, k = listed_column(col, q)
        top = (row == 0) & (p == 0)
        i = jnp.where(top, LOWER, ROWS - 1 - row)
        return live & takes & (top | (row >= ROWS - LOWER)), i, k

    for s in range(SLOTS):
        wanted, i, k = place(s)

        @pl.when(wanted)
        def _():
            here[i, k] = 1
            pltpu.make_async_copy(tiles.at[0, 0, s], held.at[k, i], sems.at[k, i]).start()

    for i in range(LOWER + 1):
        for k in range(LISTED):

            @pl.when(here[i, k] == 0)
            def _():
                held[k, i] = jnp.zeros((SIDE, SIDE), BF)

    piv = spread_rows(pivots[...])
    lane, sub = iota(1), iota(0)
    leaves = ((piv // SIDE) % N_ROW != 0) & (p == 0)
    picks = [hot(piv - SIDE * (p + N_ROW * (ROWS - 1 - i)) == lane) for i in range(LOWER)]
    picks.append(hot(jnp.where(leaves, sub, piv - SIDE * p) == lane))
    pick = jnp.concatenate(picks, axis=1)

    for k in range(LISTED):
        for i in range(LOWER + 1):

            @pl.when(here[i, k] == 1)
            def _():
                pltpu.make_async_copy(tiles.at[0, 0, 0], held.at[k, i], sems.at[k, i]).wait()

        rows = times(pick, held[k].reshape((LOWER + 1) * SIDE, SIDE)).astype(BF)
        out[:, k * CHUNK : (k + 1) * CHUNK] = rows.reshape(N_PLANE, CHUNK, SIDE)


def chunk_owner(pivots):
    first = (lax.axis_index("y") * 2 + lax.axis_index("core")) * CHUNK
    sub = iota(0, CHUNK)
    owner = jnp.zeros((CHUNK, SIDE), jnp.int32)
    for r in range(CHUNK):
        owner = jnp.where(sub == r, (pivots[first + r] // SIDE) % N_ROW, owner)
    return (owner // 2) % 2 == lax.axis_index("zh"), owner // 4 * 2 + owner % 2


def cross_kernel(pivots, got, upper, out):
    near, place = chunk_owner(pivots)
    frm = iota(1, CHUNK)
    pick = hot((iota(0, CHUNK) == frm % CHUNK) & (frm // CHUNK == jnp.where(near, place, 0)))
    for k in range(LISTED):
        out[k * CHUNK : (k + 1) * CHUNK] = times(pick, block_rows(got, k)).astype(BF)
    out[GIVEN:] = upper[...]


def wide(v):
    return jnp.broadcast_to(v[None], (N_PLANE, CHUNK, SIDE)).reshape(SIDE, SIDE)


def relay_plan(pivots):
    near, place = chunk_owner(pivots)
    near, place = wide(jnp.where(near, 1, 0)) == 1, wide(place)
    mine = iota(0) // CHUNK == place
    far = jnp.logical_not(near) | (mine & (lax.axis_index("zh") == 1))
    return far, jnp.where(mine, 0, place)


def near_kernel(pivots, got, out):
    far, source = relay_plan(pivots)
    to, frm = iota(0), iota(1)
    pick = hot((to % CHUNK == frm % CHUNK) & (frm // CHUNK == source) & jnp.logical_not(far))
    for k in range(LISTED):
        out[k] = times(pick, block_rows(got, k)).astype(BF)


def relay_kernel(pivots, near, theirs, upper, out):
    zh = lax.axis_index("zh")
    far, _ = relay_plan(pivots)
    for k in range(LISTED):
        other = wide(theirs[k * CHUNK : (k + 1) * CHUNK].astype(F32))
        rows = jnp.where(far, other, near[k].astype(F32)).astype(BF)
        out[:, k * CHUNK : (k + 1) * CHUNK] = rows.reshape(N_PLANE, CHUNK, SIDE)
    ours, others = upper[...].astype(F32), theirs[GIVEN:].astype(F32)
    for h in range(2):
        rows = jnp.where(zh == h, ours, others).astype(BF)
        out[:, GIVEN + h * PIECE : GIVEN + (h + 1) * PIECE] = jnp.broadcast_to(
            rows[None], (N_PLANE, PIECE, SIDE)
        )


def swap_plan(pivots, first):
    match = pivots - first == iota(0)
    return hot(match), jnp.max(jnp.where(match, 1.0, 0.0), axis=1, keepdims=True) > 0.0


def swap_in(plan, old, tile):
    return jnp.where(plan[1], times(plan[0], old), tile.astype(F32)).astype(BF)


def solve_kernel(ids, counts, pivots, tiles, got, *rest):
    outs, (inverse, old, held, swapped, here, sems, olds, inverses) = rest[:N_X], rest[N_X:]
    p, q = row_of(), col_of()

    @pl.when(q == 0)
    def _():
        copies = []
        for j in range(N_PLANE):
            rows = pl.ds(j * CHUNK, CHUNK)
            copies.append(
                pltpu.make_async_copy(got.at[j, pl.ds(UPPER * CHUNK, CHUNK)], old.at[rows], olds.at[j])
            )
        for j in range(N_ROW):
            y, h, c = j // 4, j // 2 % 2, j % 2
            rows = pl.ds(GIVEN + h * PIECE, PIECE)
            copies.append(
                pltpu.make_async_copy(
                    got.at[2 * y + c, rows], inverse.at[pl.ds(j * PIECE, PIECE)], inverses.at[j]
                )
            )
        for i in range(LOWER + 1):
            here[i] = 0
        for s in range(SLOTS):
            row, col, live = slot_of(ids, counts, s)
            top = (row == 0) & (p == 0)
            i = jnp.where(top, LOWER, ROWS - 1 - row)

            @pl.when(live & (col == 0) & (top | (row >= ROWS - LOWER)))
            def _():
                here[i] = 1
                pltpu.make_async_copy(tiles.at[0, 0, s], held.at[i], sems.at[i]).start()

        for copy in copies:
            copy.start()
        piv = jnp.broadcast_to(pivots[...], (SIDE, SIDE))
        plans = [swap_plan(piv, SIDE * (p + N_ROW * (ROWS - 1 - i))) for i in range(LOWER)]
        for copy in copies[:N_PLANE]:
            copy.wait()

        @pl.when(here[LOWER] == 1)
        def _():
            pltpu.make_async_copy(tiles.at[0, 0, 0], held.at[LOWER], sems.at[LOWER]).wait()
            old[...] = held[LOWER]

        for i in range(LOWER):

            @pl.when(here[i] == 1)
            def _():
                pltpu.make_async_copy(tiles.at[0, 0, 0], held.at[i], sems.at[i]).wait()

            @pl.when(here[i] == 0)
            def _():
                held[i] = jnp.zeros((SIDE, SIDE), BF)

        for i in range(LOWER):
            swapped[i * SIDE : (i + 1) * SIDE] = swap_in(plans[i], old[...], held[i])
        for copy in copies[N_PLANE:]:
            copy.wait()
        solved = times(swapped[...], inverse[...]).astype(BF)
        for i in range(LOWER):
            for c in range(N_X):
                a = i * SIDE + c * PART
                outs[c][i * PART : (i + 1) * PART] = solved[a : a + PART]


def fan_kernel(part, pieces, sent, out):
    odd = lax.axis_index("zl") % 2 == 1
    rows = jnp.where(odd, sent[:PANEL].astype(F32), part[...].astype(F32)).astype(BF)
    for c in range(N_X):
        out[c, :PANEL] = rows
        out[c, PANEL : PANEL + PART // 2] = pieces[...]
        out[c, PANEL + PART // 2 :] = sent[PANEL:]


def ready_kernel(ids, counts, pivots, tiles, gave, got, l0, l1, l2, l3, out, new, old):
    lower = (l0, l1, l2, l3)
    p, q = row_of(), col_of()
    piv = jnp.broadcast_to(pivots[...], (SIDE, SIDE))
    own = (spread_rows(pivots[...]) // SIDE) % N_ROW == p
    for k in range(LISTED):
        theirs = block_rows(got, k)
        ours = block_rows(gave, k)
        old[k] = theirs
        new[k] = jnp.where(own, ours.astype(F32), theirs.astype(F32)).astype(BF)

    def top(s, carry):
        row, col, live = slot_of(ids, counts, s)
        takes, k = listed_column(col, q)

        @pl.when(live & takes & (row == 0) & (p == 0))
        def _():
            old[k] = tiles[0, 0, s]

        return carry

    lax.fori_loop(0, SLOTS, top, 0)

    def step(s, carry):
        row, col, live = slot_of(ids, counts, s)
        takes, k = listed_column(col, q)
        first = (col == 0) & (q == 0)
        is_top = live & (row == 0) & (p == 0)
        is_lower = live & first & jnp.logical_not(is_top)
        is_swap = live & takes & jnp.logical_not(first) & (row >= ROWS - LOWER)
        is_kept = live & jnp.logical_not(is_top | is_lower | is_swap)

        @pl.when(is_top & first)
        def _():
            out[s] = new[UPPER]

        @pl.when(is_lower)
        def _():
            start = pl.multiple_of(jnp.clip(ROWS - 1 - row, 0, LOWER - 1) * PART, PART)
            for c in range(N_X):
                out[s, c * PART : (c + 1) * PART] = lower[c][pl.ds(start, PART)]

        @pl.when(is_swap)
        def _():
            out[s] = swap_in(swap_plan(piv, SIDE * (p + N_ROW * row)), old[k], tiles[0, 0, s])

        @pl.when(is_kept)
        def _():
            out[s] = tiles[0, 0, s]

        @pl.when(jnp.logical_not(live))
        def _():
            out[s] = jnp.zeros((SIDE, SIDE), BF)

        return carry

    lax.fori_loop(0, SLOTS, step, 0)


def trail_kernel(ids, counts, ready, new, panel, out, held, left, upper, sems, back):
    p = row_of()

    def place(s):
        row, col, live = slot_of(ids, counts, s)
        listed = live & (col >= COLS - UPPER)
        top = listed & (row == 0) & (p == 0)
        i = jnp.clip(ROWS - 1 - row, 0, LOWER - 1)
        k = jnp.clip(COLS - 1 - col, 0, UPPER - 1)
        return top, listed & (row >= ROWS - LOWER), i, k

    for s in range(SLOTS):
        _, trails, _, _ = place(s)

        @pl.when(trails)
        def _():
            pltpu.make_async_copy(ready.at[0, 0, s], held.at[s], sems.at[s]).start()

    j = iota(1)
    e, t = j // COLS % N_Z, j % COLS
    e = (e % 2) * 4 + e // 2 % 2 * 2 + e // 4
    mine = j // PART * PART + COLS * (e ^ lax.axis_index("zl")) + t
    pieces = panel[:, PANEL:].reshape(SIDE, SIDE)
    inverse = times(hot(mine == iota(0)), pieces).astype(BF)
    for k in range(UPPER):
        upper[k] = lax.dot_general(
            inverse, new[k], (((0,), (0,)), ((), ())), preferred_element_type=F32
        ).astype(BF)
    for i in range(LOWER):
        left[i] = panel[:, i * PART : (i + 1) * PART].reshape(SIDE, SIDE)

    for s in range(SLOTS):
        top, trails, i, k = place(s)

        @pl.when(top)
        def _():
            held[s] = upper[k]

        @pl.when(trails)
        def _():
            pltpu.make_async_copy(ready.at[0, 0, s], held.at[s], sems.at[s]).wait()
            held[s] = (held[s].astype(F32) - times(left[i], upper[k])).astype(BF)

        @pl.when(top | trails)
        def _():
            pltpu.make_async_copy(held.at[s], out.at[0, 0, s], back.at[s]).start()

    for s in range(SLOTS):
        top, trails, _, _ = place(s)

        @pl.when(top | trails)
        def _():
            pltpu.make_async_copy(held.at[s], out.at[0, 0, s], back.at[s]).wait()


def call(kernel, specs, ins, shapes, scratch=(), out_space=VMEM, aliases=None, kept=True):
    shapes = [pltpu.VMEM(o, BF) if kept else jax.ShapeDtypeStruct(o, BF) for o in shapes]
    several = len(shapes) > 1
    ins = [
        pltpu.with_memory_space_constraint(a, pltpu.VMEM) if c == "v" else a
        for c, a in zip(specs, ins, strict=True)
    ]
    return pl.pallas_call(
        kernel,
        out_shape=shapes if several else shapes[0],
        in_specs=[{"s": SMEM, "v": VMEM, "w": VMEM, "a": ANY}[c] for c in specs],
        out_specs=[out_space] * len(shapes) if several else out_space,
        scratch_shapes=list(scratch),
        input_output_aliases=aliases or {},
        name=kernel.__name__,
    )(*ins)


def body(tiles, tile_ids, counts, pivots, l_inverse, u_inverse):
    x = lax.axis_index("x")
    z = lax.axis_index("zl")
    lanes = pivots[None]
    tile = (SIDE, SIDE)
    plane = ("y", "core")

    gave = call(
        give_kernel,
        "sswa",
        [tile_ids, counts, lanes, tiles],
        [(N_PLANE, GIVEN, SIDE)],
        [
            pltpu.VMEM((LISTED, LOWER + 1, SIDE, SIDE), BF),
            pltpu.SMEM((LOWER + 1, LISTED), jnp.int32),
            pltpu.SemaphoreType.DMA((LISTED, LOWER + 1)),
        ],
    )
    got = lax.all_to_all(gave, plane, 0, 0, tiled=True)
    crossing = call(cross_kernel, "svw", [pivots, got, u_inverse], [(GIVEN + PIECE, SIDE)])
    theirs = lax.ppermute(crossing, "zh", [(0, 1), (1, 0)])
    near = call(near_kernel, "sv", [pivots, got], [(LISTED, SIDE, SIDE)])
    relayed = call(
        relay_kernel, "svvw", [pivots, near, theirs, u_inverse], [(N_PLANE, SENT, SIDE)]
    )
    have = lax.all_to_all(relayed, plane, 0, 0, tiled=True)
    have, pieces = lax.optimization_barrier((have, l_inverse.T))

    parts = call(
        solve_kernel,
        "sswaa",
        [tile_ids, counts, lanes, tiles, have],
        [(PANEL, SIDE)] * N_X,
        [
            pltpu.VMEM(tile, BF),
            pltpu.VMEM(tile, BF),
            pltpu.VMEM((LOWER + 1, SIDE, SIDE), BF),
            pltpu.VMEM((LOWER * SIDE, SIDE), BF),
            pltpu.SMEM((LOWER + 1,), jnp.int32),
            pltpu.SemaphoreType.DMA((LOWER + 1,)),
            pltpu.SemaphoreType.DMA((N_PLANE,)),
            pltpu.SemaphoreType.DMA((N_ROW,)),
        ],
    )
    part = parts[0]
    for c in range(1, N_X):
        sent = lax.ppermute(parts[c], PCOL, [(0, c * N_Z)])
        part = jnp.where(x == c, sent, part)
    first = part
    for step in (4, 2):
        more = lax.ppermute(pieces, "zl", [(a, a ^ step) for a in range(N_Z)])
        pieces = jnp.concatenate([pieces, more], axis=0)
    for to in (6, 4, 2):
        sent = lax.ppermute(first, "zl", [(0, to)])
        part = jnp.where(z == to, sent, part)
    block = jnp.concatenate([part, pieces], axis=0)
    sent = lax.ppermute(block, "zl", [(a, a ^ 1) for a in range(N_Z)])
    fan = call(fan_kernel, "vvv", [part, pieces, sent], [(N_X, SIDE, SIDE)])
    panel = lax.all_to_all(fan, "x", 0, 0, tiled=True)

    ready, new = call(
        ready_kernel,
        "sswwwwwwww",
        [tile_ids, counts, lanes, tiles, gave, have, *parts],
        [(SLOTS, SIDE, SIDE), (LISTED, SIDE, SIDE)],
        [pltpu.VMEM((LISTED, SIDE, SIDE), BF)],
        kept=False,
    )
    return call(
        trail_kernel,
        "ssawv",
        [tile_ids, counts, ready[None, None], new, panel],
        [(1, 1, SLOTS, SIDE, SIDE)],
        [
            pltpu.VMEM((SLOTS, SIDE, SIDE), BF),
            pltpu.VMEM((LOWER, SIDE, SIDE), BF),
            pltpu.VMEM((UPPER, SIDE, SIDE), BF),
            pltpu.SemaphoreType.DMA((SLOTS,)),
            pltpu.SemaphoreType.DMA((SLOTS,)),
        ],
        out_space=ANY,
        aliases={2: 0},
        kept=False,
    )


def solution(mesh):
    torus = Mesh(mesh.devices.reshape(N_Y, 2, 2, N_X, N_Z), PROW + PCOL)
    placed = (
        P(PROW, PCOL, None, None, None),
        P(PROW, PCOL, None),
        P(PROW, PCOL),
        P(),
        P(None, PCOL),
        P(PROW, None),
    )
    return jax.shard_map(
        body,
        mesh=torus,
        in_specs=placed,
        out_specs=P(PROW, PCOL, None, None, None),
        check_vma=False,
    )
```

```python
import jax
import jax.numpy as jnp
from jax import lax
from jax.experimental import pallas as pl
from jax.experimental.pallas import tpu as pltpu
from jax.sharding import Mesh
from jax.sharding import PartitionSpec as P

SIDE = 256
SLOTS = 16
ROWS = 16
COLS = 8
LOWER = 3
UPPER = 3
LISTED = UPPER + 1
N_ROW = 16
N_Y = 4
N_PLANE = 8
N_X = 4
N_Z = 8
CHUNK = SIDE // N_PLANE
PIECE = SIDE // N_ROW
PART = SIDE // N_X
GIVEN = LISTED * CHUNK
SENT = GIVEN + 2 * PIECE
PANEL = LOWER * PART
PROW = ("y", "zh", "core")
PCOL = ("x", "zl")
EVERY = PROW + PCOL
MIDDLE = 4
GATHER = ([(0, 1), (3, 2), (5, 4), (7, 6)], [(1, 2), (6, 4)], [(2, 4)])
NEAR = ([(MIDDLE, 1)], [(MIDDLE, 6)])
LAST = ([(1, 2), (4, 5), (6, 7)], [(1, 0), (4, 3)])

BF = jnp.bfloat16
F32 = jnp.float32

SMEM = pl.BlockSpec(memory_space=pltpu.SMEM)
VMEM = pl.BlockSpec(memory_space=pltpu.VMEM)
ANY = pl.BlockSpec(memory_space=pl.ANY)


def iota(dim, rows=SIDE):
    return lax.broadcasted_iota(jnp.int32, (rows, SIDE), dim)


def hot(mask):
    return jnp.where(mask, 1.0, 0.0).astype(BF)


def times(a, b):
    return jnp.dot(a, b, preferred_element_type=F32)


def row_of():
    return (lax.axis_index("y") * 2 + lax.axis_index("zh")) * 2 + lax.axis_index("core")


def col_of():
    return lax.axis_index("x") * N_Z + lax.axis_index("zl")


def slot_of(ids, counts, s):
    code = ids[0, 0, s]
    return code // COLS, code % COLS, s < counts[0, 0]


def listed_column(col, q):
    return (col >= COLS - UPPER) | ((col == 0) & (q == 0)), jnp.where(col == 0, UPPER, COLS - 1 - col)


def spread_rows(pivots):
    return jnp.transpose(jnp.broadcast_to(pivots, (SIDE, SIDE)))


def block_rows(block, k):
    return block[:, k * CHUNK : (k + 1) * CHUNK].reshape(SIDE, SIDE)


def first_kernel(ids, counts, tiles, out, sem):
    @pl.when((row_of() == 0) & (col_of() == 0))
    def _():
        for s in range(SLOTS):
            row, col, live = slot_of(ids, counts, s)

            @pl.when(live & (row == 0) & (col == 0))
            def _():
                copy = pltpu.make_async_copy(tiles.at[0, 0, s], out, sem)
                copy.start()
                copy.wait()


def give_kernel(ids, counts, pivots, tiles, out, held, here, sems):
    p, q = row_of(), col_of()
    for i in range(LOWER + 1):
        for k in range(LISTED):
            here[i, k] = 0

    def place(s):
        row, col, live = slot_of(ids, counts, s)
        takes, k = listed_column(col, q)
        top = (row == 0) & (p == 0)
        i = jnp.where(top, LOWER, ROWS - 1 - row)
        return live & takes & (top | (row >= ROWS - LOWER)), i, k

    for s in range(SLOTS):
        wanted, i, k = place(s)

        @pl.when(wanted)
        def _():
            here[i, k] = 1
            pltpu.make_async_copy(tiles.at[0, 0, s], held.at[k, i], sems.at[k, i]).start()

    for i in range(LOWER + 1):
        for k in range(LISTED):

            @pl.when(here[i, k] == 0)
            def _():
                held[k, i] = jnp.zeros((SIDE, SIDE), BF)

    piv = spread_rows(pivots[...])
    lane, sub = iota(1), iota(0)
    leaves = ((piv // SIDE) % N_ROW != 0) & (p == 0)
    picks = [hot(piv - SIDE * (p + N_ROW * (ROWS - 1 - i)) == lane) for i in range(LOWER)]
    picks.append(hot(jnp.where(leaves, sub, piv - SIDE * p) == lane))
    pick = jnp.concatenate(picks, axis=1)

    for k in range(LISTED):
        for i in range(LOWER + 1):

            @pl.when(here[i, k] == 1)
            def _():
                pltpu.make_async_copy(tiles.at[0, 0, 0], held.at[k, i], sems.at[k, i]).wait()

        rows = times(pick, held[k].reshape((LOWER + 1) * SIDE, SIDE)).astype(BF)
        out[:, k * CHUNK : (k + 1) * CHUNK] = rows.reshape(N_PLANE, CHUNK, SIDE)


def chunk_owner(pivots):
    first = (lax.axis_index("y") * 2 + lax.axis_index("core")) * CHUNK
    sub = iota(0, CHUNK)
    owner = jnp.zeros((CHUNK, SIDE), jnp.int32)
    for r in range(CHUNK):
        owner = jnp.where(sub == r, (pivots[first + r] // SIDE) % N_ROW, owner)
    return (owner // 2) % 2 == lax.axis_index("zh"), owner // 4 * 2 + owner % 2


def cross_kernel(pivots, got, upper, out):
    near, place = chunk_owner(pivots)
    frm = iota(1, CHUNK)
    pick = hot((iota(0, CHUNK) == frm % CHUNK) & (frm // CHUNK == jnp.where(near, place, 0)))
    for k in range(LISTED):
        out[k * CHUNK : (k + 1) * CHUNK] = times(pick, block_rows(got, k)).astype(BF)
    out[GIVEN:] = upper[...]


def wide(v):
    return jnp.broadcast_to(v[None], (N_PLANE, CHUNK, SIDE)).reshape(SIDE, SIDE)


def relay_plan(pivots):
    near, place = chunk_owner(pivots)
    near, place = wide(jnp.where(near, 1, 0)) == 1, wide(place)
    mine = iota(0) // CHUNK == place
    far = jnp.logical_not(near) | (mine & (lax.axis_index("zh") == 1))
    return far, jnp.where(mine, 0, place)


def near_kernel(pivots, got, out):
    far, source = relay_plan(pivots)
    to, frm = iota(0), iota(1)
    pick = hot((to % CHUNK == frm % CHUNK) & (frm // CHUNK == source) & jnp.logical_not(far))
    for k in range(LISTED):
        out[k] = times(pick, block_rows(got, k)).astype(BF)


def relay_kernel(pivots, near, theirs, upper, out):
    zh = lax.axis_index("zh")
    far, _ = relay_plan(pivots)
    for k in range(LISTED):
        other = wide(theirs[k * CHUNK : (k + 1) * CHUNK].astype(F32))
        rows = jnp.where(far, other, near[k].astype(F32)).astype(BF)
        out[:, k * CHUNK : (k + 1) * CHUNK] = rows.reshape(N_PLANE, CHUNK, SIDE)
    ours, others = upper[...].astype(F32), theirs[GIVEN:].astype(F32)
    for h in range(2):
        rows = jnp.where(zh == h, ours, others).astype(BF)
        out[:, GIVEN + h * PIECE : GIVEN + (h + 1) * PIECE] = jnp.broadcast_to(
            rows[None], (N_PLANE, PIECE, SIDE)
        )


def swap_plan(pivots, first):
    match = pivots - first == iota(0)
    return hot(match), jnp.max(jnp.where(match, 1.0, 0.0), axis=1, keepdims=True) > 0.0


def swap_in(plan, old, tile):
    return jnp.where(plan[1], times(plan[0], old), tile.astype(F32)).astype(BF)


def swap_kernel(ids, counts, pivots, tiles, old, *rest):
    outs, (held, here, sems) = rest[:N_X], rest[N_X:]
    p, q = row_of(), col_of()

    @pl.when(q == 0)
    def _():
        for i in range(LOWER):
            here[i] = 0
        for s in range(SLOTS):
            row, col, live = slot_of(ids, counts, s)
            i = ROWS - 1 - row

            @pl.when(live & (col == 0) & (row >= ROWS - LOWER))
            def _():
                here[i] = 1
                pltpu.make_async_copy(tiles.at[0, 0, s], held.at[i], sems.at[i]).start()

        piv = jnp.broadcast_to(pivots[...], (SIDE, SIDE))
        for i in range(LOWER):
            plan = swap_plan(piv, SIDE * (p + N_ROW * (ROWS - 1 - i)))

            @pl.when(here[i] == 1)
            def _():
                pltpu.make_async_copy(tiles.at[0, 0, 0], held.at[i], sems.at[i]).wait()

            @pl.when(here[i] == 0)
            def _():
                held[i] = jnp.zeros((SIDE, SIDE), BF)

            swapped = swap_in(plan, old[...], held[i])
            for c in range(N_X):
                outs[c][i * PART : (i + 1) * PART] = swapped[c * PART : (c + 1) * PART]


def fan_kernel(block, out):
    for c in range(N_X):
        out[c] = block[...]


def ready_kernel(ids, counts, pivots, tiles, gave, got, out, new, old):
    p, q = row_of(), col_of()
    piv = jnp.broadcast_to(pivots[...], (SIDE, SIDE))
    own = (spread_rows(pivots[...]) // SIDE) % N_ROW == p
    for k in range(LISTED):
        theirs = block_rows(got, k)
        ours = block_rows(gave, k)
        old[k] = theirs
        new[k] = jnp.where(own, ours.astype(F32), theirs.astype(F32)).astype(BF)

    for y in range(N_Y):
        for h in range(2):
            for c in range(2):
                r = (4 * y + 2 * h + c) * PIECE
                a = GIVEN + h * PIECE
                new[LISTED, r : r + PIECE] = got[2 * y + c, a : a + PIECE]

    def top(s, carry):
        row, col, live = slot_of(ids, counts, s)
        takes, k = listed_column(col, q)

        @pl.when(live & takes & (row == 0) & (p == 0))
        def _():
            old[k] = tiles[0, 0, s]

        return carry

    lax.fori_loop(0, SLOTS, top, 0)

    def step(s, carry):
        row, col, live = slot_of(ids, counts, s)
        takes, k = listed_column(col, q)
        first = (col == 0) & (q == 0)
        is_top = live & (row == 0) & (p == 0)
        is_lower = live & first & jnp.logical_not(is_top)
        is_swap = live & takes & jnp.logical_not(first) & (row >= ROWS - LOWER)
        is_kept = live & jnp.logical_not(is_top | is_lower | is_swap)

        @pl.when(is_top & first)
        def _():
            out[s] = new[UPPER]

        @pl.when(is_swap)
        def _():
            out[s] = swap_in(swap_plan(piv, SIDE * (p + N_ROW * row)), old[k], tiles[0, 0, s])

        @pl.when(is_kept)
        def _():
            out[s] = tiles[0, 0, s]

        @pl.when(jnp.logical_not(live))
        def _():
            out[s] = jnp.zeros((SIDE, SIDE), BF)

        return carry

    lax.fori_loop(0, SLOTS, step, 0)


def trail_kernel(ids, counts, ready, new, panel, out, held, left, upper, sems, back):
    p, q = row_of(), col_of()

    def place(s):
        row, col, live = slot_of(ids, counts, s)
        listed = live & (col >= COLS - UPPER)
        top = listed & (row == 0) & (p == 0)
        i = jnp.clip(ROWS - 1 - row, 0, LOWER - 1)
        k = jnp.clip(COLS - 1 - col, 0, UPPER - 1)
        solved = live & (col == 0) & (q == 0) & (row >= ROWS - LOWER)
        return top, listed & (row >= ROWS - LOWER), solved, i, k

    for s in range(SLOTS):
        _, trails, _, _, _ = place(s)

        @pl.when(trails)
        def _():
            pltpu.make_async_copy(ready.at[0, 0, s], held.at[s], sems.at[s]).start()

    j = iota(1)
    e, t = j // COLS % N_Z, j % COLS
    e = jnp.where(e < 4, e + 4, jnp.where(e < 6, e - 2, 7 - e))
    mine = j // PART * PART + COLS * e + t
    pieces = panel[:, PANEL:].reshape(SIDE, SIDE)
    inverse = times(hot(mine == iota(0)), pieces).astype(BF)
    for k in range(UPPER):
        upper[k] = lax.dot_general(
            inverse, new[k], (((0,), (0,)), ((), ())), preferred_element_type=F32
        ).astype(BF)
    for i in range(LOWER):
        swapped = panel[:, i * PART : (i + 1) * PART].reshape(SIDE, SIDE)
        left[i] = times(swapped, new[LISTED]).astype(BF)

    for s in range(SLOTS):
        top, trails, solved, i, k = place(s)

        @pl.when(top)
        def _():
            held[s] = upper[k]

        @pl.when(solved)
        def _():
            held[s] = left[i]

        @pl.when(trails)
        def _():
            pltpu.make_async_copy(ready.at[0, 0, s], held.at[s], sems.at[s]).wait()
            held[s] = (held[s].astype(F32) - times(left[i], upper[k])).astype(BF)

        @pl.when(top | trails | solved)
        def _():
            pltpu.make_async_copy(held.at[s], out.at[0, 0, s], back.at[s]).start()

    for s in range(SLOTS):
        top, trails, solved, _, _ = place(s)

        @pl.when(top | trails | solved)
        def _():
            pltpu.make_async_copy(held.at[s], out.at[0, 0, s], back.at[s]).wait()


def call(kernel, specs, ins, shapes, scratch=(), out_space=VMEM, aliases=None, kept=True):
    shapes = [pltpu.VMEM(o, BF) if kept else jax.ShapeDtypeStruct(o, BF) for o in shapes]
    several = len(shapes) > 1
    ins = [
        pltpu.with_memory_space_constraint(a, pltpu.VMEM) if c == "v" else a
        for c, a in zip(specs, ins, strict=True)
    ]
    return pl.pallas_call(
        kernel,
        out_shape=shapes if several else shapes[0],
        in_specs=[{"s": SMEM, "v": VMEM, "w": VMEM, "a": ANY}[c] for c in specs],
        out_specs=[out_space] * len(shapes) if several else out_space,
        scratch_shapes=list(scratch),
        input_output_aliases=aliases or {},
    )(*ins)


def device(y, zh, core):
    return ((y * 2 + zh) * 2 + core) * N_X * N_Z


def body(tiles, tile_ids, counts, pivots, l_inverse, u_inverse):
    y, zh, core, x, z = (lax.axis_index(a) for a in EVERY)
    lanes = pivots[None]
    tile = (SIDE, SIDE)
    plane = ("y", "core")

    pieces = l_inverse.T
    for pairs in GATHER:
        more = lax.ppermute(pieces, "zl", pairs)
        pieces = jnp.concatenate([pieces, more], axis=0)

    first = call(
        first_kernel, "ssa", [tile_ids, counts, tiles], [tile], [pltpu.SemaphoreType.DMA]
    )
    old = first
    for to in range(1, N_Y):
        sent = lax.ppermute(first, EVERY, [(device(0, 0, 0), device(to, 0, 0))])
        old = jnp.where(y == to, sent, old)
    sent = lax.ppermute(old, EVERY, [(device(a, 0, 0), device(a, 0, 1)) for a in range(N_Y)])
    old = jnp.where(core == 1, sent, old)
    sent = lax.ppermute(
        old, EVERY, [(device(a, 0, c), device(a, 1, c)) for a in range(N_Y) for c in range(2)]
    )
    old = jnp.where(zh == 1, sent, old)

    gave = call(
        give_kernel,
        "sswa",
        [tile_ids, counts, lanes, tiles],
        [(N_PLANE, GIVEN, SIDE)],
        [
            pltpu.VMEM((LISTED, LOWER + 1, SIDE, SIDE), BF),
            pltpu.SMEM((LOWER + 1, LISTED), jnp.int32),
            pltpu.SemaphoreType.DMA((LISTED, LOWER + 1)),
        ],
    )
    got = lax.all_to_all(gave, plane, 0, 0, tiled=True)

    parts = call(
        swap_kernel,
        "sswav",
        [tile_ids, counts, lanes, tiles, old],
        [(PANEL, SIDE)] * N_X,
        [
            pltpu.VMEM((LOWER, SIDE, SIDE), BF),
            pltpu.SMEM((LOWER,), jnp.int32),
            pltpu.SemaphoreType.DMA((LOWER,)),
        ],
    )
    arrived = [lax.ppermute(parts[c], PCOL, [(0, c * N_Z + MIDDLE)]) for c in range(N_X)]

    crossing = call(cross_kernel, "svw", [pivots, got, u_inverse], [(GIVEN + PIECE, SIDE)])
    theirs = lax.ppermute(crossing, "zh", [(0, 1), (1, 0)])
    near = call(near_kernel, "sv", [pivots, got], [(LISTED, SIDE, SIDE)])
    relayed = call(
        relay_kernel, "svvw", [pivots, near, theirs, u_inverse], [(N_PLANE, SENT, SIDE)]
    )
    have = lax.all_to_all(relayed, plane, 0, 0, tiled=True)

    part = arrived[0]
    for c in range(1, N_X):
        part = jnp.where(x == c, arrived[c], part)
    block = jnp.concatenate([part, pieces], axis=0)
    for stage in (NEAR, LAST):
        sent = [lax.ppermute(block, "zl", pairs) for pairs in stage]
        for pairs, there in zip(stage, sent, strict=True):
            for _, to in pairs:
                block = jnp.where(z == to, there, block)
    fan = call(fan_kernel, "v", [block], [(N_X, SIDE, SIDE)])
    panel = lax.all_to_all(fan, "x", 0, 0, tiled=True)

    ready, new = call(
        ready_kernel,
        "sswwww",
        [tile_ids, counts, lanes, tiles, gave, have],
        [(SLOTS, SIDE, SIDE), (LISTED + 1, SIDE, SIDE)],
        [pltpu.VMEM((LISTED, SIDE, SIDE), BF)],
        kept=False,
    )
    return call(
        trail_kernel,
        "ssawv",
        [tile_ids, counts, ready[None, None], new, panel],
        [(1, 1, SLOTS, SIDE, SIDE)],
        [
            pltpu.VMEM((SLOTS, SIDE, SIDE), BF),
            pltpu.VMEM((LOWER, SIDE, SIDE), BF),
            pltpu.VMEM((UPPER, SIDE, SIDE), BF),
            pltpu.SemaphoreType.DMA((SLOTS,)),
            pltpu.SemaphoreType.DMA((SLOTS,)),
        ],
        out_space=ANY,
        aliases={2: 0},
        kept=False,
    )


def solution(mesh):
    torus = Mesh(mesh.devices.reshape(N_Y, 2, 2, N_X, N_Z), PROW + PCOL)
    placed = (
        P(PROW, PCOL, None, None, None),
        P(PROW, PCOL, None),
        P(PROW, PCOL),
        P(),
        P(None, PCOL),
        P(PROW, None),
    )
    return jax.shard_map(
        body,
        mesh=torus,
        in_specs=placed,
        out_specs=P(PROW, PCOL, None, None, None),
        check_vma=False,
    )
```
